32 devices in a mesh: row: 8 (over z, x), col: 4 (over y, core).
Axes of the slice: x: 2, y: 2, z: 4, core: 2. Of those that a mesh axis runs over, the one named last changes fastest.
Arguments:
- curvature: float32 [32, 1024, 4096], P(None, 'row', 'col'), may hold values from -4 to 7, as said below
Outputs:
- factored: float32 [32, 1024, 4096], P(None, 'row', 'col')
The draws below stay inside these ranges and needn't reach their ends.
Inputs may be any that keep to these rules, and one draw needn't show every extreme that they name: `curvature`: rows 0 to 4095, read as a square matrix, are symmetric positive definite with smallest eigenvalue at least 0.5.
All inputs are finite; a program needn't handle non-finite values.
Results may differ from the reference program's by a relative error of at most 0.0014.
Values may be sent and summed in bfloat16 or wider, within the bound.
A program may use at most 192 MiB of HBM per device.

```python
import math
import jax
import jax.numpy as jnp
from jax import lax

MATRIX = 32768
PANEL = 1024
STEPS = 2
CYCLES = 32
N_COL = 4


def draw_curvature(key, part):
    slab_width = N_COL * PANEL
    gram_rows = slab_width // 2
    key_jacobian = jax.random.fold_in(key, 101)
    key_bottom = jax.random.fold_in(key, 202)
    key_damping = jax.random.fold_in(key, 303)
    jacobian = jnp.clip(jax.random.normal(key_jacobian, (gram_rows, slab_width), jnp.float32), -4.0, 4.0)
    bottom = jnp.clip(jax.random.normal(key_bottom, (MATRIX - slab_width, slab_width), jnp.float32), -4.0, 4.0)
    gram = jnp.dot(jacobian.T, jacobian, precision=lax.Precision.HIGHEST, preferred_element_type=jnp.float32) / gram_rows
    gram = 0.5 * (gram + gram.T)
    damping = jnp.exp(jax.random.uniform(key_damping, (slab_width,), jnp.float32, math.log(0.5), math.log(2.0)))
    identity = jnp.eye(slab_width, dtype=jnp.float32)
    top_block = gram + identity * damping[None, :]
    whole = jnp.concatenate([top_block, bottom], 0)
    return whole.reshape(MATRIX // PANEL, PANEL, slab_width)


def setup_inputs(seed: int = 0) -> dict:
    splits = jax.random.split(jax.random.key(seed), 2)
    curvature = draw_curvature(jax.random.fold_in(splits[1], 71), 0)
    return dict(curvature=curvature)


def reference(curvature):
    slab_width = N_COL * PANEL
    matrix = curvature.reshape(MATRIX, slab_width)
    for step in range(STEPS):
        lower_edge = step * PANEL
        upper_edge = lower_edge + PANEL
        factor = jnp.linalg.cholesky(matrix[lower_edge:upper_edge, lower_edge:upper_edge])
        solved = jax.scipy.linalg.solve_triangular(factor, matrix[upper_edge:, lower_edge:upper_edge].T, lower=True).T
        panel_new = jnp.concatenate([jnp.zeros((lower_edge, PANEL), matrix.dtype), factor, solved], 0)
        matrix = matrix.at[:, lower_edge:upper_edge].set(panel_new)
        rounded = lax.optimization_barrier(solved.astype(jnp.bfloat16)).astype(jnp.float32)
        update = jnp.dot(rounded.astype(jnp.float32), rounded[:slab_width - upper_edge].T.astype(jnp.float32), precision=lax.Precision.HIGHEST, preferred_element_type=jnp.float32)
        matrix = matrix.at[upper_edge:, upper_edge:].add(-update)
    row_ids = lax.broadcasted_iota(jnp.int32, (MATRIX, slab_width), 0)
    col_ids = lax.broadcasted_iota(jnp.int32, (MATRIX, slab_width), 1)
    blanked = (row_ids < STEPS * PANEL) & (col_ids >= STEPS * PANEL)
    matrix = jnp.where(blanked, jnp.zeros_like(matrix), matrix)
    return matrix.reshape(CYCLES, PANEL, slab_width)
```

```python
import functools

import jax
import jax.numpy as jnp
from jax import lax
from jax.experimental import pallas as pl
from jax.experimental.pallas import tpu as pltpu
from jax.sharding import PartitionSpec as P


BLOCK, STRIP = 128, 16
HIGHEST = lax.Precision.HIGHEST
F32, BF16 = jnp.float32, jnp.bfloat16
NN, NT, TN = ((1,), (0,)), ((1,), (1,)), ((0,), (0,))


def dot(left, right, dims=NN, precision=None):
    return lax.dot_general(left, right, (dims, ((), ())), precision=precision, preferred_element_type=F32)


def factor_small(work, strip):
    size = work.shape[0]
    lane = lax.broadcasted_iota(jnp.int32, (strip, size), 1)
    sub = lax.broadcasted_iota(jnp.int32, (strip, size), 0)
    done, diag = [], []
    for at in range(0, size, strip):
        head = work[:strip]
        columns = [jnp.broadcast_to(head[:, at + j : at + j + 1], (strip, size)) for j in range(strip)]
        inside = (lane >= at) & (lane < at + strip)
        wide = jnp.where(inside, jnp.where(lane - at == sub, 1.0, 0.0), head)
        pivots = jnp.ones((strip, size), F32)
        for k in range(strip):
            pivot = jnp.broadcast_to(columns[k][k : k + 1], (strip, size))
            pivots = jnp.where(sub == k, pivot, pivots)
            if k < strip - 1:
                scale = jnp.where(sub > k, columns[k] * (1.0 / pivot), 0.0)
                for j in range(k + 1, strip):
                    columns[j] = columns[j] - scale * jnp.broadcast_to(columns[j][k : k + 1], (strip, size))
                wide = wide - scale * jnp.broadcast_to(wide[k : k + 1], (strip, size))
        root = lax.rsqrt(pivots)
        wide = wide * root
        own = jnp.zeros((strip, size), F32)
        for j in range(strip):
            own = jnp.where((lane == at + j) & (sub <= j), columns[j], own)
        diag.append(own * root)
        done.append(wide)
        if at + strip < size:
            rest = size - at - strip
            low = jnp.where(jnp.broadcast_to(inside[:1], (rest, size)), 0.0, work[strip:])
            work = low - dot(wide, wide, TN, HIGHEST)[at + strip :]
    return jnp.concatenate(done, 0), jnp.concatenate(diag, 0)


HALVES = 2


def gather_kernel(columns, x_ref, out_ref, send_sem, recv_sem):
    n_row, col = lax.axis_size("row"), lax.axis_index("col")
    row = lax.axis_index("row")
    half = n_row // 2
    odd = row % 2
    at = (1 - odd) * (row // 2) + odd * (n_row - 1 - row // 2)

    def neighbour(by):
        p = (at + by + n_row) % n_row
        late = p // half
        return {"row": (1 - late) * 2 * p + late * (2 * (n_row - 1 - p) + 1)}

    mesh_id = pl.DeviceIdType.MESH
    size = x_ref.shape[0] // HALVES

    @pl.when((col >= columns[0]) & (col <= columns[-1]) & ((col - columns[0]) % columns[1] == 0))
    def _():
        barrier = pltpu.get_barrier_semaphore()
        for by in (1, -1):
            pl.semaphore_signal(barrier, inc=1, device_id=neighbour(by), device_id_type=mesh_id)
        pl.semaphore_wait(barrier, 2)
        copies = {}
        for k in range(1, half + 1):
            for h in range(HALVES):
                rows = pl.ds(h * size, size)
                for by in (1, -1):
                    slot = 2 * k - 1 if by == 1 else 2 * k
                    if slot >= n_row:
                        continue
                    source = x_ref.at[rows] if k == 1 else out_ref.at[slot - 2, rows]
                    if k > 1:
                        copies[slot - 2, h].wait_recv()
                    copies[slot, h] = pltpu.make_async_remote_copy(
                        src_ref=source,
                        dst_ref=out_ref.at[slot, rows],
                        send_sem=send_sem.at[slot, h],
                        recv_sem=recv_sem.at[slot, h],
                        device_id=neighbour(by),
                        device_id_type=mesh_id,
                    )
                    copies[slot, h].start()
        out_ref[0] = x_ref[...]
        for (slot, h), copy in copies.items():
            copy.wait_send()
            if slot >= n_row - 2:
                copy.wait_recv()


def gather(x, columns, collective_id, n_row):
    vmem = pl.BlockSpec(memory_space=pltpu.VMEM)
    return pl.pallas_call(
        functools.partial(gather_kernel, columns),
        out_shape=jax.ShapeDtypeStruct((n_row, *x.shape), x.dtype),
        in_specs=[vmem],
        out_specs=vmem,
        scratch_shapes=[pltpu.SemaphoreType.DMA((n_row, HALVES)), pltpu.SemaphoreType.DMA((n_row, HALVES))],
        compiler_params=pltpu.CompilerParams(
            collective_id=collective_id, has_side_effects=True, vmem_limit_bytes=16 << 20
        ),
        cost_estimate=pl.CostEstimate(flops=10**9, bytes_accessed=8 * n_row * x.size, transcendentals=0),
    )(x)


def place(out_ref, pieces_ref, order_ref):
    count, tile, _ = pieces_ref.shape
    for i in range(count):
        out_ref[pl.ds(pl.multiple_of(order_ref[2 + i] * tile, tile), tile), :] = pieces_ref[i]


def factor_kernel(which, order_ref, tops, *refs):
    faces, refs = (refs[0], refs[1:]) if which else (None, refs)
    mixed_ref, diag_ref, high_ref, low_ref = refs[:4]
    half_ref = refs[-1]
    n = mixed_ref.shape[0]
    block = diag_ref.shape[1]
    strip = min(STRIP, block)
    count = n // block
    sub = lax.broadcasted_iota(jnp.int32, (block, block), 0)
    lane = lax.broadcasted_iota(jnp.int32, (block, block), 1)

    def rows(b):
        return pl.ds(pl.multiple_of(b * block, block), block)

    def subtract(b, carry):
        face_ref = refs[4]
        mixed_ref[rows(b), :] = mixed_ref[rows(b), :] - dot(face_ref[rows(b), :], face_ref[...], NT)
        return carry

    def step(b, carry):
        here = rows(b)
        inner, diag = factor_small(mixed_ref[here, here], strip)
        diag_ref[here, :] = jnp.where(lane // strip > sub // strip, inner, 0.0) + diag
        mixed_ref[here, here] = jnp.where(sub == lane, 1.0, 0.0)
        half_ref[...] = dot(jnp.where(sub >= lane, inner, 0.0), mixed_ref[here, :], NN, HIGHEST)
        mixed_ref[here, :] = half_ref[...]

        def lower(i, carry):
            low = rows(i)
            mixed_ref[low, here] = jnp.zeros((block, block), F32)
            mixed_ref[low, :] = mixed_ref[low, :] - dot(half_ref[:, low], half_ref[...], TN, HIGHEST)
            return carry

        return lax.fori_loop(b + 1, count, lower, carry)

    def emit(b, carry):
        at = lax.broadcasted_iota(jnp.int32, (block, n), 0) + b * block
        inverse = jnp.where(lax.broadcasted_iota(jnp.int32, (block, n), 1) <= at, mixed_ref[rows(b), :], 0.0)
        high_ref[rows(b), :], low_ref[rows(b), :] = split(inverse)
        return carry

    if which:

        @pl.when(order_ref[0] > 0)
        def _():
            place(refs[4], faces, order_ref)

    @pl.when(order_ref[0] == which)
    def _():
        place(mixed_ref, tops, order_ref)
        if which:
            lax.fori_loop(0, count, subtract, 0)
        lax.fori_loop(0, count, step, 0)
        lax.fori_loop(0, count, emit, 0)


def factor(order, tops, faces):
    n = tops.shape[2]
    block = min(BLOCK, n)
    vmem = pl.BlockSpec(memory_space=pltpu.VMEM)
    which = len(faces)
    shapes = [((n, n), F32), ((n, block), F32), ((n, n), BF16), ((n, n), BF16)] + [((n, n), BF16)] * which
    return pl.pallas_call(
        functools.partial(factor_kernel, which),
        out_shape=[jax.ShapeDtypeStruct(*s) for s in shapes],
        in_specs=[pl.BlockSpec(memory_space=pltpu.SMEM)] + [vmem] * (1 + which),
        out_specs=[vmem] * len(shapes),
        scratch_shapes=[pltpu.VMEM((block, n), F32)],
        compiler_params=pltpu.CompilerParams(vmem_limit_bytes=32 << 20),
        cost_estimate=pl.CostEstimate(flops=20 * n**3, bytes_accessed=8 * n * n, transcendentals=0),
    )(order, tops, *faces)


def assemble_kernel(order_ref, pieces_ref, out_ref):
    place(out_ref, pieces_ref, order_ref)


def assemble(order, pieces):
    n = pieces.shape[2]
    vmem = pl.BlockSpec(memory_space=pltpu.VMEM)
    return pl.pallas_call(
        assemble_kernel,
        out_shape=jax.ShapeDtypeStruct((n, n), pieces.dtype),
        in_specs=[pl.BlockSpec(memory_space=pltpu.SMEM), vmem],
        out_specs=vmem,
        name="assemble",
    )(order, pieces)


def split(x):
    high = x.astype(BF16)
    return high, (x - high.astype(F32)).astype(BF16)


def times_inverse(rows, high_ref, low_ref):
    n = rows.shape[1]
    piece = min(256, n)
    high, low = split(rows)
    outs = []
    for at in range(0, n, piece):
        k, here = at + piece, pl.ds(at, piece)
        right = high_ref[here, :k]
        outs.append(
            dot(high[:, :k], right, NT) + (dot(low[:, :k], right, NT) + dot(high[:, :k], low_ref[here, :k], NT))
        )
    return jnp.concatenate(outs, 1)


def solve_kernel(role_ref, m_ref, high_ref, low_ref, solved_ref, sent_ref):
    @pl.when(role_ref[0] > 0)
    def _():
        tiles, tile, n = m_ref.shape
        solved = times_inverse(m_ref[...].reshape(tiles * tile, n), high_ref, low_ref).reshape(m_ref.shape)
        solved_ref[...] = solved
        sent_ref[...] = solved.astype(BF16)


def second_kernel(role_ref, m_ref, p_ref, f_ref, high_ref, low_ref, solved_ref, sent_ref):
    @pl.when(role_ref[0] > 0)
    def _():
        tiles, tile, n = m_ref.shape
        rows = tiles * tile
        m = m_ref[...].reshape(rows, n) - dot(p_ref[...].reshape(rows, n), f_ref[...], NT)
        solved = times_inverse(m, high_ref, low_ref).reshape(m_ref.shape)
        solved_ref[...] = solved
        sent_ref[...] = solved.astype(BF16)


def whole(x):
    return pl.BlockSpec(x.shape, lambda i, role: (0,) * x.ndim, pipeline_mode=pl.Buffered(1))


def panel_call(body, active, curvature, first, tiles, before, weights, passes):
    _, tile, n = curvature.shape
    deep = 2 if tiles % 2 == 0 else 1
    block = (deep, tile, n)
    steps = tiles // deep
    at = first // deep
    inner = pl.BlockSpec(block, lambda i, role: (i * role[0], 0, 0))
    return pl.pallas_call(
        body,
        out_shape=(jax.ShapeDtypeStruct((tiles, tile, n), F32), jax.ShapeDtypeStruct((tiles, tile, n), BF16)),
        grid_spec=pltpu.PrefetchScalarGridSpec(
            num_scalar_prefetch=1,
            grid=(steps,),
            in_specs=[pl.BlockSpec(block, lambda i, role: (at + i * role[0], 0, 0))]
            + [inner] * len(before)
            + [whole(w) for w in weights],
            out_specs=[inner, inner],
        ),
        compiler_params=pltpu.CompilerParams(vmem_limit_bytes=40 << 20, dimension_semantics=("arbitrary",)),
        cost_estimate=pl.CostEstimate(
            flops=2 * passes * tiles * tile * n * n, bytes_accessed=10 * tiles * tile * n, transcendentals=0
        ),
    )(active, curvature, *before, *weights)


def top_kernel(role_ref, mixed0_ref, diag0_ref, mixed1_ref, diag1_ref, edge_ref, out_ref, turned_ref):
    tile, n = edge_ref.shape[1:]
    block = diag0_ref.shape[0]
    here = role_ref[2]

    def own_rows(mixed_ref, diag_ref):
        at = lax.broadcasted_iota(jnp.int32, (n, block), 0) // block
        turned_ref[...] = jnp.where(at < here, mixed_ref[...], 0.0).T
        turned_ref[:, pl.ds(pl.multiple_of(here * block, block), block)] = diag_ref[...].T
        return turned_ref[pl.ds(pl.multiple_of(role_ref[3], tile), tile), :]

    out_ref[...] = jnp.zeros_like(out_ref)

    @pl.when(role_ref[0] == 0)
    def _():
        out_ref[0] = own_rows(mixed0_ref, diag0_ref)
        out_ref[1] = edge_ref[0]

    @pl.when(role_ref[0] == 1)
    def _():
        out_ref[1] = own_rows(mixed1_ref, diag1_ref)


def place_top(role, mixed0, diag0, mixed1, diag1, edge, shape):
    _, tile, n = edge.shape
    block = diag0.shape[1]
    side = pl.BlockSpec((n, block), lambda i, role: (0, role[2]))
    inner = pl.BlockSpec((block, block), lambda i, role: (role[2], 0))
    return pl.pallas_call(
        top_kernel,
        out_shape=jax.ShapeDtypeStruct(shape, F32),
        grid_spec=pltpu.PrefetchScalarGridSpec(
            num_scalar_prefetch=1,
            grid=(1,),
            in_specs=[side, inner, side, inner, pl.BlockSpec(edge.shape, lambda i, role: (0, 0, 0))],
            out_specs=pl.BlockSpec((2, tile, n), lambda i, role: (0, 0, 0)),
            scratch_shapes=[pltpu.VMEM((block, n), F32)],
        ),
        cost_estimate=pl.CostEstimate(flops=10**8, bytes_accessed=8 * tile * n, transcendentals=0),
        name="top",
    )(role, mixed0, diag0, mixed1, diag1, edge)


def finish_kernel(role_ref, m_ref, s0_ref, s1_ref, p0a_ref, p0b_ref, p1a_ref, p1b_ref, f0_ref, f1_ref, _, out_ref):
    col = role_ref[0]
    tiles, tile, n = m_ref.shape
    rows = tiles * tile

    @pl.when(col == 0)
    def _():
        out_ref[...] = s0_ref[...]

    @pl.when(col == 1)
    def _():
        out_ref[...] = s1_ref[...]

    def update(p0_ref, p1_ref):
        total = dot(p0_ref[...].reshape(rows, n), f0_ref[...], NT) + dot(p1_ref[...].reshape(rows, n), f1_ref[...], NT)
        out_ref[...] = m_ref[...] - total.reshape(m_ref.shape)

    @pl.when((col > 1) & (role_ref[1] == 0))
    def _():
        update(p0a_ref, p1a_ref)

    @pl.when((col > 1) & (role_ref[1] == 1))
    def _():
        update(p0b_ref, p1b_ref)


def finish(role, curvature, first, tiles, s0, s1, p0, p1, f0, f1, out):
    _, tile, n = curvature.shape
    block = (2, tile, n)
    at = first // 2

    def pick(test):
        return pl.BlockSpec(block, lambda i, role: (jnp.where(test(role), i, 0), 0, 0))

    low = lambda role: (role[0] > 1) & (role[1] == 0)
    high = lambda role: (role[0] > 1) & (role[1] == 1)
    return pl.pallas_call(
        finish_kernel,
        out_shape=jax.ShapeDtypeStruct(curvature.shape, F32),
        grid_spec=pltpu.PrefetchScalarGridSpec(
            num_scalar_prefetch=1,
            grid=(tiles // 2,),
            in_specs=[
                pl.BlockSpec(block, lambda i, role: (at + jnp.where(role[0] > 1, i, 0), 0, 0)),
                pick(lambda role: role[0] == 0),
                pick(lambda role: role[0] == 1),
                pick(low),
                pick(high),
                pick(low),
                pick(high),
                whole(f0),
                whole(f1),
                pl.BlockSpec(memory_space=pl.ANY),
            ],
            out_specs=pl.BlockSpec(block, lambda i, role: (at + i, 0, 0)),
        ),
        input_output_aliases={10: 0},
        compiler_params=pltpu.CompilerParams(vmem_limit_bytes=40 << 20, dimension_semantics=("arbitrary",)),
        cost_estimate=pl.CostEstimate(
            flops=4 * tiles * tile * n * n, bytes_accessed=12 * tiles * tile * n, transcendentals=0
        ),
        name="finish",
    )(role, curvature, s0, s1, *p0, *p1, f0, f1, out)


def factored(curvature):
    cycles, tile, _ = curvature.shape
    row, col = lax.axis_index("row"), lax.axis_index("col")
    n_row, n_col = lax.axis_size("row"), lax.axis_size("col")
    as_flag = lambda test: jnp.reshape(test.astype(jnp.int32), (1,))
    role = jnp.stack([col, col % 2]).astype(jnp.int32)
    cycle = list(range(0, n_row, 2)) + list(range(1, n_row, 2))[::-1]
    place_in_cycle = jnp.array([cycle.index(r) for r in range(n_row)], jnp.int32)[row]
    steps = [0] + [s for k in range(1, n_row // 2 + 1) for s in ([k, -k] if 2 * k < n_row else [k])]
    sources = jnp.array(cycle, jnp.int32)[(place_in_cycle - jnp.array(steps, jnp.int32)) % n_row]
    order = jnp.concatenate([role, sources])

    def send(x, pairs):
        return lax.ppermute(x, "col", pairs)

    def onward(x, source):
        got = send(x, [(source, source + 2)])
        for hop in range(4, n_col, 2):
            further = send(got, [(source + hop - 2, source + hop)])
            got = jnp.where(col == source + hop, further, got)
        across = send(got, [(hop + source, hop + 1 - source) for hop in range(2, n_col, 2)])
        return (got, across) if source == 0 else (across, got)

    def facing_tile(tiles, first):
        return lax.dynamic_index_in_dim(tiles, jnp.clip(col - first, 0, tiles.shape[0] - 1), 0, False)

    blocks = (cycles - n_col) // 2
    per = 2 * -(-blocks // 4)
    spans = [(2, n_col - 2)] + [(at, min(per, cycles - at)) for at in range(n_col, cycles, per)]

    aside = send(curvature[1], [(1, 3)])
    tops0 = gather(jnp.where(col == 3, aside, curvature[0]), (0, 3, 3), 0, n_row)
    tops1 = send(tops0, [(3, 1)])
    mixed0, diag0, high0, low0 = factor(order, tops0, [])

    def solve(first, tiles):
        return panel_call(solve_kernel, as_flag(col == 0), curvature, first, tiles, [], [high0, low0], 3)

    edge_solved, edge = solve(1, 1)
    edge = send(edge, [(0, 1)])[0]
    s0, p0_next, p0 = [], [], []
    for first, tiles in spans:
        solved, sent = solve(first, tiles)
        s0.append(solved)
        p0.append(onward(sent, 0))
        p0_next.append(send(sent, [(0, 1)]))
    faces0 = jnp.where(col % 2 == 0, facing_tile(p0[0][0], 2), facing_tile(p0[0][1], 2))
    faces0 = gather(jnp.where(col == 1, edge, faces0), (1, 1, n_col - 1), 1, n_row)
    mixed1, diag1, high1, low1, facing0 = factor(order, tops1, [faces0])

    s1, p1 = [], []
    for k, (first, tiles) in enumerate(spans):
        solved, sent = panel_call(
            second_kernel, as_flag(col == 1), curvature, first, tiles, [p0_next[k]], [facing0, high1, low1], 4
        )
        s1.append(solved)
        p1.append(onward(sent, 1))
    faces1 = jnp.where(col % 2 == 0, facing_tile(p1[0][0], 2), facing_tile(p1[0][1], 2))
    faces1 = gather(faces1, (2, 1, n_col - 1), 2, n_row)
    facing1 = assemble(order, faces1)

    wide = diag0.shape[1]
    places = jnp.stack([col, col % 2, row * tile // wide, row * tile % wide]).astype(jnp.int32)
    out = place_top(places, mixed0, diag0, mixed1, diag1, edge_solved, curvature.shape)
    for k, (first, tiles) in enumerate(spans):
        out = finish(role, curvature, first, tiles, s0[k], s1[k], p0[k], p1[k], facing0, facing1, out)
    return out


def solution(mesh):
    spec = P(None, "row", "col")
    return jax.shard_map(factored, mesh=mesh, in_specs=(spec,), out_specs=spec, check_vma=False)
```

```python
import functools

import jax
import jax.numpy as jnp
from jax import lax
from jax.experimental import pallas as pl
from jax.experimental.pallas import tpu as pltpu
from jax.sharding import PartitionSpec as P


BLOCK, STRIP = 128, 16
HIGHEST = lax.Precision.HIGHEST
F32, BF16 = jnp.float32, jnp.bfloat16
NN, NT, TN = ((1,), (0,)), ((1,), (1,)), ((0,), (0,))


def dot(left, right, dims=NN, precision=None):
    return lax.dot_general(left, right, (dims, ((), ())), precision=precision, preferred_element_type=F32)


def factor_small(work, strip):
    size = work.shape[0]
    lane = lax.broadcasted_iota(jnp.int32, (strip, size), 1)
    sub = lax.broadcasted_iota(jnp.int32, (strip, size), 0)
    done, diag = [], []
    for at in range(0, size, strip):
        head = work[:strip]
        columns = [jnp.broadcast_to(head[:, at + j : at + j + 1], (strip, size)) for j in range(strip)]
        inside = (lane >= at) & (lane < at + strip)
        wide = jnp.where(inside, jnp.where(lane - at == sub, 1.0, 0.0), head)
        pivots = jnp.ones((strip, size), F32)
        for k in range(strip):
            pivot = jnp.broadcast_to(columns[k][k : k + 1], (strip, size))
            pivots = jnp.where(sub == k, pivot, pivots)
            if k < strip - 1:
                scale = jnp.where(sub > k, columns[k] * (1.0 / pivot), 0.0)
                for j in range(k + 1, strip):
                    columns[j] = columns[j] - scale * jnp.broadcast_to(columns[j][k : k + 1], (strip, size))
                wide = wide - scale * jnp.broadcast_to(wide[k : k + 1], (strip, size))
        root = lax.rsqrt(pivots)
        wide = wide * root
        own = jnp.zeros((strip, size), F32)
        for j in range(strip):
            own = jnp.where((lane == at + j) & (sub <= j), columns[j], own)
        diag.append(own * root)
        done.append(wide)
        if at + strip < size:
            rest = size - at - strip
            low = jnp.where(jnp.broadcast_to(inside[:1], (rest, size)), 0.0, work[strip:])
            work = low - dot(wide, wide, TN, HIGHEST)[at + strip :]
    return jnp.concatenate(done, 0), jnp.concatenate(diag, 0)


HALVES = 2


def gather_kernel(columns, x_ref, out_ref, send_sem, recv_sem):
    n_row, col = lax.axis_size("row"), lax.axis_index("col")
    row = lax.axis_index("row")
    half = n_row // 2
    odd = row % 2
    at = (1 - odd) * (row // 2) + odd * (n_row - 1 - row // 2)

    def neighbour(by):
        p = (at + by + n_row) % n_row
        late = p // half
        return {"row": (1 - late) * 2 * p + late * (2 * (n_row - 1 - p) + 1)}

    mesh_id = pl.DeviceIdType.MESH
    size = x_ref.shape[0] // HALVES

    @pl.when((col >= columns[0]) & (col <= columns[-1]) & ((col - columns[0]) % columns[1] == 0))
    def _():
        barrier = pltpu.get_barrier_semaphore()
        for by in (1, -1):
            pl.semaphore_signal(barrier, inc=1, device_id=neighbour(by), device_id_type=mesh_id)
        pl.semaphore_wait(barrier, 2)
        copies = {}
        for k in range(1, half + 1):
            for h in range(HALVES):
                rows = pl.ds(h * size, size)
                for by in (1, -1):
                    slot = 2 * k - 1 if by == 1 else 2 * k
                    if slot >= n_row:
                        continue
                    source = x_ref.at[rows] if k == 1 else out_ref.at[slot - 2, rows]
                    if k > 1:
                        copies[slot - 2, h].wait_recv()
                    copies[slot, h] = pltpu.make_async_remote_copy(
                        src_ref=source,
                        dst_ref=out_ref.at[slot, rows],
                        send_sem=send_sem.at[slot, h],
                        recv_sem=recv_sem.at[slot, h],
                        device_id=neighbour(by),
                        device_id_type=mesh_id,
                    )
                    copies[slot, h].start()
        out_ref[0] = x_ref[...]
        for (slot, h), copy in copies.items():
            copy.wait_send()
            if slot >= n_row - 2:
                copy.wait_recv()


def gather(x, columns, collective_id, n_row):
    vmem = pl.BlockSpec(memory_space=pltpu.VMEM)
    return pl.pallas_call(
        functools.partial(gather_kernel, columns),
        out_shape=jax.ShapeDtypeStruct((n_row, *x.shape), x.dtype),
        in_specs=[vmem],
        out_specs=vmem,
        scratch_shapes=[pltpu.SemaphoreType.DMA((n_row, HALVES)), pltpu.SemaphoreType.DMA((n_row, HALVES))],
        compiler_params=pltpu.CompilerParams(
            collective_id=collective_id, has_side_effects=True, vmem_limit_bytes=16 << 20
        ),
        cost_estimate=pl.CostEstimate(flops=10**9, bytes_accessed=8 * n_row * x.size, transcendentals=0),
    )(x)


def place(out_ref, pieces_ref, order_ref):
    count, tile, _ = pieces_ref.shape
    for i in range(count):
        out_ref[pl.ds(pl.multiple_of(order_ref[2 + i] * tile, tile), tile), :] = pieces_ref[i]


def factor_kernel(which, order_ref, tops, *refs):
    faces, refs = (refs[0], refs[1:]) if which else (None, refs)
    mixed_ref, diag_ref, high_ref, low_ref = refs[:4]
    half_ref = refs[-1]
    n = mixed_ref.shape[0]
    block = diag_ref.shape[1]
    strip = min(STRIP, block)
    count = n // block
    sub = lax.broadcasted_iota(jnp.int32, (block, block), 0)
    lane = lax.broadcasted_iota(jnp.int32, (block, block), 1)

    def rows(b):
        return pl.ds(pl.multiple_of(b * block, block), block)

    def subtract(b, carry):
        face_ref = refs[4]
        mixed_ref[rows(b), :] = mixed_ref[rows(b), :] - dot(face_ref[rows(b), :], face_ref[...], NT)
        return carry

    def step(b, carry):
        here = rows(b)
        inner, diag = factor_small(mixed_ref[here, here], strip)
        diag_ref[here, :] = jnp.where(lane // strip > sub // strip, inner, 0.0) + diag
        mixed_ref[here, here] = jnp.where(sub == lane, 1.0, 0.0)
        half_ref[...] = dot(jnp.where(sub >= lane, inner, 0.0), mixed_ref[here, :], NN, HIGHEST)
        mixed_ref[here, :] = half_ref[...]

        def lower(i, carry):
            low = rows(i)
            mixed_ref[low, here] = jnp.zeros((block, block), F32)
            mixed_ref[low, :] = mixed_ref[low, :] - dot(half_ref[:, low], half_ref[...], TN, HIGHEST)
            return carry

        return lax.fori_loop(b + 1, count, lower, carry)

    def emit(b, carry):
        at = lax.broadcasted_iota(jnp.int32, (block, n), 0) + b * block
        inverse = jnp.where(lax.broadcasted_iota(jnp.int32, (block, n), 1) <= at, mixed_ref[rows(b), :], 0.0)
        high_ref[rows(b), :], low_ref[rows(b), :] = split(inverse)
        return carry

    if which:

        @pl.when(order_ref[0] > 0)
        def _():
            place(refs[4], faces, order_ref)

    @pl.when(order_ref[0] == which)
    def _():
        place(mixed_ref, tops, order_ref)
        if which:
            lax.fori_loop(0, count, subtract, 0)
        lax.fori_loop(0, count, step, 0)
        lax.fori_loop(0, count, emit, 0)


def factor(order, tops, faces):
    n = tops.shape[2]
    block = min(BLOCK, n)
    vmem = pl.BlockSpec(memory_space=pltpu.VMEM)
    which = len(faces)
    shapes = [((n, n), F32), ((n, block), F32), ((n, n), BF16), ((n, n), BF16)] + [((n, n), BF16)] * which
    return pl.pallas_call(
        functools.partial(factor_kernel, which),
        out_shape=[jax.ShapeDtypeStruct(*s) for s in shapes],
        in_specs=[pl.BlockSpec(memory_space=pltpu.SMEM)] + [vmem] * (1 + which),
        out_specs=[vmem] * len(shapes),
        scratch_shapes=[pltpu.VMEM((block, n), F32)],
        compiler_params=pltpu.CompilerParams(vmem_limit_bytes=32 << 20),
        cost_estimate=pl.CostEstimate(flops=20 * n**3, bytes_accessed=8 * n * n, transcendentals=0),
    )(order, tops, *faces)


def assemble_kernel(order_ref, pieces_ref, out_ref):
    place(out_ref, pieces_ref, order_ref)


def assemble(order, pieces):
    n = pieces.shape[2]
    vmem = pl.BlockSpec(memory_space=pltpu.VMEM)
    return pl.pallas_call(
        assemble_kernel,
        out_shape=jax.ShapeDtypeStruct((n, n), pieces.dtype),
        in_specs=[pl.BlockSpec(memory_space=pltpu.SMEM), vmem],
        out_specs=vmem,
        name="assemble",
    )(order, pieces)


def split(x):
    high = x.astype(BF16)
    return high, (x - high.astype(F32)).astype(BF16)


def times_inverse(rows, high_ref, low_ref):
    n = rows.shape[1]
    piece = min(256, n)
    high, low = split(rows)
    outs = []
    for at in range(0, n, piece):
        k, here = at + piece, pl.ds(at, piece)
        right = high_ref[here, :k]
        outs.append(
            dot(high[:, :k], right, NT) + (dot(low[:, :k], right, NT) + dot(high[:, :k], low_ref[here, :k], NT))
        )
    return jnp.concatenate(outs, 1)


def solve_kernel(role_ref, m_ref, high_ref, low_ref, *outs):
    solved_ref, sent_ref = outs[-2:]

    @pl.when(role_ref[0] > 0)
    def _():
        tiles, tile, n = m_ref.shape
        solved = times_inverse(m_ref[...].reshape(tiles * tile, n), high_ref, low_ref).reshape(m_ref.shape)
        solved_ref[...] = solved
        sent_ref[...] = solved.astype(BF16)


def second_kernel(role_ref, m_ref, p_ref, f_ref, high_ref, low_ref, *outs):
    solved_ref, sent_ref = outs[-2:]

    @pl.when(role_ref[0] > 0)
    def _():
        tiles, tile, n = m_ref.shape
        rows = tiles * tile
        m = m_ref[...].reshape(rows, n) - dot(p_ref[...].reshape(rows, n), f_ref[...], NT)
        solved = times_inverse(m, high_ref, low_ref).reshape(m_ref.shape)
        solved_ref[...] = solved
        sent_ref[...] = solved.astype(BF16)


def whole(x):
    return pl.BlockSpec(x.shape, lambda i, role: (0,) * x.ndim, pipeline_mode=pl.Buffered(1))


def panel_call(body, active, curvature, first, tiles, before, weights, out, passes):
    _, tile, n = curvature.shape
    deep = 2 if tiles % 2 == 0 else 1
    block = (deep, tile, n)
    at = first // deep
    inner = pl.BlockSpec(block, lambda i, role: (i * role[0], 0, 0))
    chained = [] if out is None else [out]
    shape, spec = curvature.shape, pl.BlockSpec(block, lambda i, role: ((at + i) * role[0], 0, 0))
    if deep == 1:
        shape, spec = (tiles, tile, n), inner
    return pl.pallas_call(
        body,
        out_shape=(jax.ShapeDtypeStruct(shape, F32), jax.ShapeDtypeStruct((tiles, tile, n), BF16)),
        grid_spec=pltpu.PrefetchScalarGridSpec(
            num_scalar_prefetch=1,
            grid=(tiles // deep,),
            in_specs=[pl.BlockSpec(block, lambda i, role: (at + i * role[0], 0, 0))]
            + [inner] * len(before)
            + [whole(w) for w in weights]
            + [pl.BlockSpec(memory_space=pl.ANY) for _ in chained],
            out_specs=[spec, inner],
        ),
        input_output_aliases={2 + len(before) + len(weights): 0} if chained else {},
        compiler_params=pltpu.CompilerParams(vmem_limit_bytes=40 << 20, dimension_semantics=("arbitrary",)),
        cost_estimate=pl.CostEstimate(
            flops=2 * passes * tiles * tile * n * n, bytes_accessed=10 * tiles * tile * n, transcendentals=0
        ),
    )(active, curvature, *before, *weights, *chained)


def top_kernel(role_ref, mixed0_ref, diag0_ref, mixed1_ref, diag1_ref, edge_ref, out_ref, turned_ref):
    tile, n = edge_ref.shape[1:]
    block = diag0_ref.shape[0]
    here = role_ref[2]

    def own_rows(mixed_ref, diag_ref):
        at = lax.broadcasted_iota(jnp.int32, (n, block), 0) // block
        turned_ref[...] = jnp.where(at < here, mixed_ref[...], 0.0).T
        turned_ref[:, pl.ds(pl.multiple_of(here * block, block), block)] = diag_ref[...].T
        return turned_ref[pl.ds(pl.multiple_of(role_ref[3], tile), tile), :]

    out_ref[...] = jnp.zeros_like(out_ref)

    @pl.when(role_ref[0] == 0)
    def _():
        out_ref[0] = own_rows(mixed0_ref, diag0_ref)
        out_ref[1] = edge_ref[0]

    @pl.when(role_ref[0] == 1)
    def _():
        out_ref[1] = own_rows(mixed1_ref, diag1_ref)


def place_top(role, mixed0, diag0, mixed1, diag1, edge):
    _, tile, n = edge.shape
    block = diag0.shape[1]
    side = pl.BlockSpec((n, block), lambda i, role: (0, role[2]))
    inner = pl.BlockSpec((block, block), lambda i, role: (role[2], 0))
    return pl.pallas_call(
        top_kernel,
        out_shape=jax.ShapeDtypeStruct((2, tile, n), F32),
        grid_spec=pltpu.PrefetchScalarGridSpec(
            num_scalar_prefetch=1,
            grid=(1,),
            in_specs=[side, inner, side, inner, pl.BlockSpec(edge.shape, lambda i, role: (0, 0, 0))],
            out_specs=pl.BlockSpec((2, tile, n), lambda i, role: (0, 0, 0)),
            scratch_shapes=[pltpu.VMEM((block, n), F32)],
        ),
        cost_estimate=pl.CostEstimate(flops=10**8, bytes_accessed=8 * tile * n, transcendentals=0),
        name="top",
    )(role, mixed0, diag0, mixed1, diag1, edge)


def subtract_product(role_ref, m_ref, even_ref, odd_ref, f_ref, out_ref):
    @pl.when(role_ref[0] > 1)
    def _():
        panel = jnp.where(role_ref[1] == 0, even_ref[...], odd_ref[...])
        rows = panel.reshape(-1, panel.shape[2])
        out_ref[...] = m_ref[...] - dot(rows, f_ref[...], NT).reshape(m_ref.shape)


def finish_kernel(lead, role_ref, m_ref, even_ref, odd_ref, f_ref, top_ref, _, out_ref):
    at_top = (role_ref[0] < 2) | (pl.program_id(0) < lead)

    @pl.when(at_top)
    def _():
        out_ref[...] = top_ref[...]

    @pl.when(jnp.logical_not(at_top))
    def _():
        subtract_product(role_ref, m_ref, even_ref, odd_ref, f_ref, out_ref)


def picker(block, lead=0):
    def pick(test, at=0):
        return pl.BlockSpec(block, lambda i, role: (at + jnp.where(test(role), jnp.maximum(i - lead, 0), 0), 0, 0))

    trailing = lambda role: role[0] > 1
    sides = [pick(lambda role, c=c: (role[0] > 1) & (role[1] == c)) for c in (0, 1)]
    return pick, trailing, sides


def finish_call(body, role, out_shape, in_specs, out_spec, tiles, steps, operands, alias):
    _, tile, n = out_shape.shape
    return pl.pallas_call(
        body,
        out_shape=out_shape,
        grid_spec=pltpu.PrefetchScalarGridSpec(
            num_scalar_prefetch=1, grid=(steps,), in_specs=in_specs, out_specs=out_spec
        ),
        input_output_aliases=alias,
        compiler_params=pltpu.CompilerParams(vmem_limit_bytes=40 << 20, dimension_semantics=("arbitrary",)),
        cost_estimate=pl.CostEstimate(
            flops=2 * tiles * tile * n * n, bytes_accessed=10 * tiles * tile * n, transcendentals=0
        ),
    )(role, *operands)


def half(role, curvature, first, tiles, p0, f0):
    _, tile, n = curvature.shape
    block = (2, tile, n)
    pick, trailing, sides = picker(block)
    return finish_call(
        subtract_product,
        role,
        jax.ShapeDtypeStruct((tiles, tile, n), F32),
        [pick(trailing, first // 2), *sides, whole(f0)],
        pick(trailing),
        tiles,
        tiles // 2,
        (curvature, *p0, f0),
        {},
    )


def finish(role, state, first, tiles, p1, f1, top, out):
    _, tile, n = out.shape
    block = (2, tile, n)
    at = first // 2
    lead = 1 if first == 2 else 0
    pick, trailing, sides = picker(block, lead)
    return finish_call(
        functools.partial(finish_kernel, lead),
        role,
        jax.ShapeDtypeStruct(out.shape, F32),
        [pick(trailing), *sides, whole(f1), whole(top), pl.BlockSpec(memory_space=pl.ANY)],
        pl.BlockSpec(
            block, lambda i, role: (jnp.where((role[0] > 1) & (i >= lead), at + i - lead, 0), 0, 0)
        ),
        tiles,
        tiles // 2 + lead,
        (state, *p1, f1, top, out),
        {6: 0},
    )


def factored(curvature):
    cycles, tile, _ = curvature.shape
    row, col = lax.axis_index("row"), lax.axis_index("col")
    n_row, n_col = lax.axis_size("row"), lax.axis_size("col")
    as_flag = lambda test: jnp.reshape(test.astype(jnp.int32), (1,))
    role = jnp.stack([col, col % 2]).astype(jnp.int32)
    cycle = list(range(0, n_row, 2)) + list(range(1, n_row, 2))[::-1]
    place_in_cycle = jnp.array([cycle.index(r) for r in range(n_row)], jnp.int32)[row]
    steps = [0] + [s for k in range(1, n_row // 2 + 1) for s in ([k, -k] if 2 * k < n_row else [k])]
    sources = jnp.array(cycle, jnp.int32)[(place_in_cycle - jnp.array(steps, jnp.int32)) % n_row]
    order = jnp.concatenate([role, sources])

    def send(x, pairs):
        return lax.ppermute(x, "col", pairs)

    def onward(x, source):
        got = send(x, [(source, source + 2)])
        for hop in range(4, n_col, 2):
            further = send(got, [(source + hop - 2, source + hop)])
            got = jnp.where(col == source + hop, further, got)
        across = send(got, [(hop + source, hop + 1 - source) for hop in range(2, n_col, 2)])
        return (got, across) if source == 0 else (across, got)

    def facing_tile(tiles, first):
        return lax.dynamic_index_in_dim(tiles, jnp.clip(col - first, 0, tiles.shape[0] - 1), 0, False)

    blocks = (cycles - n_col) // 2
    per = 2 * -(-blocks // 3)
    spans = [(2, n_col - 2)] + [(at, min(per, cycles - at)) for at in range(n_col, cycles, per)]

    aside = send(curvature[1], [(1, 3)])
    tops0 = gather(jnp.where(col == 3, aside, curvature[0]), (0, 3, 3), 0, n_row)
    tops1 = send(tops0, [(3, 1)])
    mixed0, diag0, high0, low0 = factor(order, tops0, [])

    def solve(first, tiles, out):
        return panel_call(solve_kernel, as_flag(col == 0), curvature, first, tiles, [], [high0, low0], out, 3)

    edge_solved, edge = solve(1, 1, None)
    edge = send(edge, [(0, 1)])[0]
    out, p0_next, p0 = None, [], []
    for first, tiles in spans:
        out, sent = solve(first, tiles, out)
        p0.append(onward(sent, 0))
        p0_next.append(send(sent, [(0, 1)]))
    faces0 = jnp.where(col % 2 == 0, facing_tile(p0[0][0], 2), facing_tile(p0[0][1], 2))
    faces0 = gather(jnp.where(col == 1, edge, faces0), (1, 1, n_col - 1), 1, n_row)
    mixed1, diag1, high1, low1, facing0 = factor(order, tops1, [faces0])

    p1 = []
    for k, (first, tiles) in enumerate(spans):
        out, sent = panel_call(
            second_kernel, as_flag(col == 1), curvature, first, tiles, [p0_next[k]], [facing0, high1, low1], out, 4
        )
        p1.append(onward(sent, 1))
    faces1 = jnp.where(col % 2 == 0, facing_tile(p1[0][0], 2), facing_tile(p1[0][1], 2))
    faces1 = gather(faces1, (2, 1, n_col - 1), 2, n_row)
    facing1 = assemble(order, faces1)

    wide = diag0.shape[1]
    places = jnp.stack([col, col % 2, row * tile // wide, row * tile % wide]).astype(jnp.int32)
    top = place_top(places, mixed0, diag0, mixed1, diag1, edge_solved)
    for k, (first, tiles) in enumerate(spans):
        state = half(role, curvature, first, tiles, p0[k], facing0)
        out = finish(role, state, first, tiles, p1[k], facing1, top, out)
    return out


def solution(mesh):
    spec = P(None, "row", "col")
    return jax.shard_map(factored, mesh=mesh, in_specs=(spec,), out_specs=spec, check_vma=False)
```
